128 devices in a mesh: dp: 4 (over z_hi, core), ctx: 32 (over z_lo, y, x).
Axes of the slice: x: 4, y: 4, z: 4 (z_hi: 2, z_lo: 2; z = z_hi * 2 + z_lo), core: 2. Of those that a mesh axis runs over, the one named last changes fastest.
Arguments:
- density: float32 [512, 64, 64], P(('dp', 'ctx')), parts along dimension 0, may hold values from 0.1 to 50, as said below
- stem_weight: bfloat16 [216, 1024], replicated, may hold values from -0.4375 to 0.4375
- stem_bias: float32 [1024], replicated, may hold values from -3 to 3
- pos_embed: bfloat16 [8192, 1024], P('ctx'), may hold values from -3 to 3
- ln1_gain: float32 [1024], replicated, may hold values from 0.25 to 1.75
- ln1_bias: float32 [1024], replicated, may hold values from -2 to 2
- w_qkv: bfloat16 [1024, 3072], replicated, may hold values from -2 to 2
- qkv_bias: float32 [3072], replicated, may hold values from -2 to 2
- w_out: bfloat16 [1024, 1024], replicated, may hold values from -0.1875 to 0.1875
- out_bias: float32 [1024], replicated, may hold values from -2 to 2
- ln2_gain: float32 [1024], replicated, may hold values from 0.25 to 1.75
- ln2_bias: float32 [1024], replicated, may hold values from -2 to 2
- w_fc1: bfloat16 [1024, 4096], replicated, may hold values from -0.1875 to 0.1875
- fc1_bias: float32 [4096], replicated, may hold values from -3 to 3
- w_fc2: bfloat16 [4096, 1024], replicated, may hold values from -0.09375 to 0.09375
- fc2_bias: float32 [1024], replicated, may hold values from -2 to 2
Outputs:
- encoded: bfloat16 [32768, 1024], P(('dp', 'ctx')), parts along dimension 0
The draws below stay inside these ranges and needn't reach their ends.
There are 4 independent parts, one for each index of `dp`. The reference program is written for one: setup_inputs(seed, part) draws one part's arguments, and reference() takes and returns one part's arrays. A program takes and returns all parts, laid end to end along the dimension named above; an argument that names none is the same for every part. Nothing has to cross between parts.
Inputs may be any that keep to these rules, and one draw needn't show every extreme that they name: density is positive.
All inputs are finite; a program needn't handle non-finite values.
Results may differ from the reference program's by a relative error of at most 0.013.
Values may be sent and summed in bfloat16 or wider, within the bound.
No kernel may reach another device: no remote copies, remote signals or barrier semaphores. Data moves between devices by JAX's collectives and lax.ppermute only.
A program may use at most 384 MiB of HBM per device.

```python
import math
import jax
import jax.numpy as jnp
from jax import lax

D = 1024
FF = 4096
HEADS = 16
KERNEL = 6
STRIDE = 4
GYZ = 16
TX = 32
TOKENS = 8192


def draw_density(key, part):
    planes = STRIDE * TX
    side_cells = STRIDE * GYZ
    key_one = jax.random.fold_in(key, 11)
    gradient = jnp.arange(planes, dtype=jnp.float32)[:, None, None] / max(planes - 1, 1)
    entries = jnp.exp(jax.random.uniform(key_one, (planes, side_cells, side_cells), jnp.float32, math.log(0.2), math.log(5.0)))
    scaling = jnp.exp(math.log(3.0) * gradient)
    return entries * scaling


def draw_w_qkv(key, part):
    key_one = jax.random.fold_in(jax.random.fold_in(key, 23), 0)
    spread = 1.6 / math.sqrt(D)
    return (jnp.clip(jax.random.normal(key_one, (D, 3 * D), jnp.float32), -6.0, 6.0) * spread).astype(jnp.bfloat16)


def block_scale(stream_key, extent, shards, low, top_value):
    def one(position, parts):
        draws = jax.random.uniform(jax.random.fold_in(jax.random.fold_in(stream_key, 6), position), (parts,), jnp.float32, low / len(shards), top_value / len(shards))
        return jnp.repeat(jnp.exp(draws), extent[position] // parts).reshape((-1,) + (1,) * (len(extent) - position - 1))

    level = one(*shards[0])
    for cut in shards[1:]:
        level = level * one(*cut)
    return level


def scatter_about(key, extent, scale, most, cuts=(), kind=jnp.bfloat16):
    gain = block_scale(key, extent, cuts, -0.22, 0.18) if cuts else 1.0
    values = jax.random.normal(key, extent, jnp.float32) * scale * gain
    return jnp.minimum(jnp.maximum(values, -most), most).astype(kind)


def setup_inputs(seed: int = 0, part: int = 0) -> dict:
    key_list = jax.random.split(jax.random.key(seed), 17)
    part_keys = jax.random.split(jax.random.fold_in(key_list[16], part), 17)
    return {
        "density": draw_density(jax.random.fold_in(jax.random.fold_in(key_list[16], part), 71), part),
        "stem_weight": scatter_about(key_list[1], (KERNEL * KERNEL * KERNEL, D), (KERNEL * KERNEL * KERNEL) ** -0.5, 0.4375),
        "stem_bias": scatter_about(key_list[2], (D,), 0.5, 3.0, (), jnp.float32),
        "pos_embed": scatter_about(key_list[3], (TOKENS, D), 0.5, 3.0, ((0, 32),)),
        "ln1_gain": jnp.clip(1.0 + 0.15 * jax.random.normal(key_list[4], (D,), jnp.float32), 0.25, 1.75),
        "ln1_bias": scatter_about(key_list[5], (D,), 0.3, 2.0, (), jnp.float32),
        "w_qkv": draw_w_qkv(jax.random.fold_in(key_list[16], 71), part),
        "qkv_bias": scatter_about(key_list[7], (3 * D,), 0.3, 2.0, (), jnp.float32),
        "w_out": scatter_about(key_list[8], (D, D), D ** -0.5, 0.1875),
        "out_bias": scatter_about(key_list[9], (D,), 0.3, 2.0, (), jnp.float32),
        "ln2_gain": jnp.clip(1.0 + 0.15 * jax.random.normal(key_list[10], (D,), jnp.float32), 0.25, 1.75),
        "ln2_bias": scatter_about(key_list[11], (D,), 0.3, 2.0, (), jnp.float32),
        "w_fc1": scatter_about(key_list[12], (D, FF), D ** -0.5, 0.1875),
        "fc1_bias": scatter_about(key_list[13], (FF,), 0.5, 3.0, (), jnp.float32),
        "w_fc2": scatter_about(key_list[14], (FF, D), FF ** -0.5, 0.09375),
        "fc2_bias": scatter_about(key_list[15], (D,), 0.3, 2.0, (), jnp.float32),
    }


def layer_norm(inputs, gain_vector, shift_vector):
    values = inputs.astype(jnp.float32)
    center = values - lax.optimization_barrier(jnp.mean(values, axis=-1, keepdims=True))
    spread = lax.optimization_barrier(jnp.mean(center * center, axis=-1, keepdims=True))
    return center * lax.rsqrt(spread + 1e-06) * gain_vector + shift_vector

def stem_conv(stacked, stem_weight):
    model_width = stem_weight.shape[1]
    kernel = stem_weight.reshape(6, 6, 6, 1, model_width)
    result = lax.conv_general_dilated(stacked[..., None], kernel, (4, 4, 4), ((1, 1), (1, 1), (1, 1)), dimension_numbers=('NDHWC', 'DHWIO', 'NDHWC'), preferred_element_type=jnp.float32)
    return result.reshape(-1, model_width)

def single_head(triple):
    query_head, key_head, value_head = triple
    scores = jnp.dot(query_head, key_head.T, preferred_element_type=jnp.float32)
    row_max = lax.optimization_barrier(jnp.max(scores, axis=1, keepdims=True))
    weights = jnp.exp(scores - row_max)
    row_total = lax.optimization_barrier(jnp.sum(weights, axis=1, keepdims=True))
    mixed = jnp.dot(weights.astype(jnp.bfloat16), value_head, preferred_element_type=jnp.float32) / row_total
    return mixed.astype(jnp.bfloat16)

def reference(density, stem_weight, stem_bias, pos_embed, ln1_gain, ln1_bias, w_qkv, qkv_bias, w_out, out_bias, ln2_gain, ln2_bias, w_fc1, fc1_bias, w_fc2, fc2_bias):
    model_width = w_out.shape[0]
    head_size = model_width // HEADS
    mean_density = jnp.mean(density)
    field = jnp.log(density / mean_density).astype(jnp.bfloat16)
    embedded = stem_conv(field[None], stem_weight) + stem_bias + pos_embed.astype(jnp.float32)
    residual = embedded.astype(jnp.bfloat16)
    normed = layer_norm(residual, ln1_gain, ln1_bias).astype(jnp.bfloat16)
    projected = jnp.dot(normed, w_qkv, preferred_element_type=jnp.float32) + qkv_bias
    token_count = normed.shape[0]
    query_rows = (projected[:, :model_width] * (1.0 / head_size ** 0.5)).astype(jnp.bfloat16)
    key_rows = projected[:, model_width:2 * model_width].astype(jnp.bfloat16)
    value_rows = projected[:, 2 * model_width:].astype(jnp.bfloat16)

    def split_heads(matrix):
        return matrix.reshape(token_count, HEADS, head_size).transpose(1, 0, 2)
    attended = lax.map(single_head, (split_heads(query_rows), split_heads(key_rows), split_heads(value_rows)))
    attended = attended.transpose(1, 0, 2).reshape(token_count, model_width)
    stream = (residual.astype(jnp.float32) + jnp.dot(attended, w_out, preferred_element_type=jnp.float32) + out_bias).astype(jnp.bfloat16)
    normed_two = layer_norm(stream, ln2_gain, ln2_bias).astype(jnp.bfloat16)
    hidden = jax.nn.gelu(jnp.dot(normed_two, w_fc1, preferred_element_type=jnp.float32) + fc1_bias, approximate=False).astype(jnp.bfloat16)
    encoded = stream.astype(jnp.float32) + jnp.dot(hidden, w_fc2, preferred_element_type=jnp.float32) + fc2_bias
    return encoded.astype(jnp.bfloat16)
```

```python
import functools
import math

import jax
import jax.numpy as jnp
from jax import lax
from jax.experimental import pallas as pl
from jax.experimental.pallas import tpu as pltpu
from jax.sharding import PartitionSpec as P

HEADS = 16
HEAD = 64
D = 1024
FF = 4096
SIDE = 16
TOK = 256
PLANE = 16
BOUND = 100.0
F32 = jnp.float32
BF16 = jnp.bfloat16


def layer_norm(values, gain, shift):
    center = values - jnp.mean(values, axis=-1, keepdims=True)
    spread = jnp.mean(center * center, axis=-1, keepdims=True)
    return center * lax.rsqrt(spread + 1e-06) * gain + shift


def front_kernel(
    sums_ref, edge_ref, low_ref, mid_ref, high_ref, pick_ref, stem_ref, sbias_ref, pos_ref,
    gain_ref, shift_ref, wqkv_ref, qbias_ref, send_ref, resid_ref, cols_ref,
):
    total = jnp.sum(sums_ref[...])
    mean = total / (32 * 4 * 64 * 64)
    planes = []
    for a in range(6):
        if a == 0:
            values = jnp.where(edge_ref[0] > 0, low_ref[0], mean)
        elif a == 5:
            values = jnp.where(edge_ref[1] > 0, high_ref[0], mean)
        else:
            values = mid_ref[a - 1]
        planes.append(jnp.log(values / mean).astype(BF16))
    field = jnp.concatenate(planes, axis=0)
    cols_ref[:, 0:8, :] = jnp.zeros((SIDE, 8, 128), F32)
    cols_ref[:, 72:80, :] = jnp.zeros((SIDE, 8, 128), F32)
    picked = lax.dot_general(
        field, pick_ref[...], (((0,), (0,)), ((), ())), preferred_element_type=F32
    )
    for j in range(SIDE):
        cols_ref[j, 8:72, :] = picked[:, j * 128 : (j + 1) * 128]
    embedded = sbias_ref[...] + pos_ref[...].astype(F32)
    for c in range(6):
        rows = [cols_ref[j, pl.ds(7 + c, SIDE, stride=4), :] for j in range(SIDE)]
        taps = jnp.concatenate(rows, axis=0).astype(BF16)
        embedded = embedded + jnp.dot(taps[:, :48], stem_ref[c], preferred_element_type=F32)
    residual = embedded.astype(BF16)
    resid_ref[...] = residual
    normed = layer_norm(residual.astype(F32), gain_ref[...], shift_ref[...]).astype(BF16)
    scale = math.log2(math.e) / math.sqrt(HEAD)
    place = (2, 0, 1)
    for part in range(3):
        for n in range(2):
            start = part * D + n * 512
            out = jnp.dot(normed, wqkv_ref[:, start : start + 512], preferred_element_type=F32)
            out = out + qbias_ref[:, start : start + 512]
            if part == 0:
                out = out * scale
            out = out.astype(BF16)
            for h in range(0, 8, 2):
                pair = out[:, h * HEAD : (h + 2) * HEAD].T
                row = place[part] * HEAD
                send_ref[n * 8 + h, row : row + HEAD, :] = pair[:HEAD]
                send_ref[n * 8 + h + 1, row : row + HEAD, :] = pair[HEAD:]


def largest_square(ref, first):
    def one(s, best):
        values = ref[s, first : first + HEAD, :].astype(F32)
        return jnp.maximum(best, jnp.sum(values * values, axis=0, keepdims=True))

    return jnp.max(lax.fori_loop(0, PLANE, one, jnp.zeros((1, TOK), F32)))


def attend_kernel(*refs, last):
    if last:
        (q_ref, kv_ref, acc_in, max_in, out_ref, k_scr, v_scr, flag) = refs
    else:
        (q_ref, acc_out, max_out, k_scr, v_scr, flag) = refs
        kv_ref = q_ref
    step = pl.program_id(0)

    @pl.when(step == 0)
    def _():
        def one(s, _):
            off = pl.multiple_of(s * TOK, TOK)
            k_scr[pl.ds(off, TOK), :] = kv_ref[s, 0:HEAD, :].T
            v_scr[0:HEAD, pl.ds(off, TOK)] = kv_ref[s, HEAD : 2 * HEAD, :]
            return 0

        lax.fori_loop(0, PLANE, one, 0)
        v_scr[HEAD : HEAD + 16, :] = jnp.ones((16, PLANE * TOK), BF16)
        reach = largest_square(kv_ref, 0) * largest_square(q_ref, 2 * HEAD)
        flag[0] = jnp.where(reach <= BOUND * BOUND, 1, 0).astype(jnp.int32)

    small = flag[0] == 1
    row = 2 * HEAD
    query = jnp.concatenate(
        [q_ref[2 * step, row : row + HEAD, :], q_ref[2 * step + 1, row : row + HEAD, :]], axis=1
    )
    width = 2 * TOK

    def finish(acc, top):
        if last:
            out = (acc[:HEAD] / acc[HEAD : HEAD + 1]).astype(BF16)
            out_ref[0] = out[:, :TOK]
            out_ref[1] = out[:, TOK:]
        else:
            acc_out[...] = acc
            max_out[...] = top

    if last:
        carried = jnp.all(max_in[...] == 0.0)
        plain = jnp.logical_and(small, carried)
    else:
        plain = small

    @pl.when(plain)
    def _():
        scores = jnp.dot(k_scr[...], query, preferred_element_type=F32)
        weights = jnp.exp2(scores).astype(BF16)
        acc = jnp.dot(v_scr[...], weights, preferred_element_type=F32)
        if last:
            acc = acc + acc_in[...]
        finish(acc, jnp.zeros((8, width), F32))

    @pl.when(jnp.logical_not(plain))
    def _():
        chunk = 256

        def one(c, carry):
            acc, top = carry
            off = pl.multiple_of(c * chunk, chunk)
            scores = jnp.dot(k_scr[pl.ds(off, chunk), :], query, preferred_element_type=F32)
            new_top = jnp.maximum(top, jnp.max(scores, axis=0, keepdims=True))
            weights = jnp.exp2(scores - new_top).astype(BF16)
            acc = acc * jnp.exp2(top - new_top) + jnp.dot(
                v_scr[:, pl.ds(off, chunk)], weights, preferred_element_type=F32
            )
            return acc, new_top

        if last:
            begin = (acc_in[...], max_in[0:1, :])
        else:
            begin = (jnp.zeros((HEAD + 16, width), F32), jnp.full((1, width), -3e38, F32))
        acc, top = lax.fori_loop(0, PLANE * TOK // chunk, one, begin)
        finish(acc, jnp.broadcast_to(top, (8, width)))


def attend(operands, last):
    width = 2 * TOK
    queries = PLANE * TOK
    whole = lambda rows: pl.BlockSpec((PLANE, rows, TOK), lambda i: (0, 0, 0))
    acc_spec = pl.BlockSpec((HEAD + 16, width), lambda i: (0, i))
    max_spec = pl.BlockSpec((8, width), lambda i: (0, i))
    if last:
        in_specs = [whole(3 * HEAD), whole(2 * HEAD), acc_spec, max_spec]
        out_specs = pl.BlockSpec((2, HEAD, TOK), lambda i: (i, 0, 0))
        out_shape = jax.ShapeDtypeStruct((PLANE, HEAD, TOK), BF16)
    else:
        in_specs = [whole(3 * HEAD)]
        out_specs = [acc_spec, max_spec]
        out_shape = [
            jax.ShapeDtypeStruct((HEAD + 16, queries), F32),
            jax.ShapeDtypeStruct((8, queries), F32),
        ]
    return pl.pallas_call(
        functools.partial(attend_kernel, last=last),
        grid=(queries // width,),
        in_specs=in_specs,
        out_specs=out_specs,
        out_shape=out_shape,
        scratch_shapes=[
            pltpu.VMEM((queries, HEAD), BF16),
            pltpu.VMEM((HEAD + 16, queries), BF16),
            pltpu.SMEM((1,), jnp.int32),
        ],
        compiler_params=pltpu.CompilerParams(vmem_limit_bytes=24 * 2**20),
        name="attend_last" if last else "attend_first",
    )(*operands)


def back_kernel(
    att_ref, resid_ref, wout_ref, obias_ref, gain_ref, shift_ref, fc1_ref, b1_ref, fc2_ref,
    b2_ref, out_ref,
):
    mixed = lax.dot_general(
        att_ref[...], wout_ref[...], (((0,), (0,)), ((), ())), preferred_element_type=F32
    )
    stream = (resid_ref[...].astype(F32) + mixed + obias_ref[...]).astype(BF16)
    wide = stream.astype(F32)
    normed = layer_norm(wide, gain_ref[...], shift_ref[...]).astype(BF16)
    acc = wide + b2_ref[...]
    chunk = 1024
    for f in range(0, FF, chunk):
        pre = jnp.dot(normed, fc1_ref[:, f : f + chunk], preferred_element_type=F32)
        pre = pre + b1_ref[:, f : f + chunk]
        hidden = (0.5 * pre * (1.0 + lax.erf(pre * math.sqrt(0.5)))).astype(BF16)
        acc = acc + jnp.dot(hidden, fc2_ref[f : f + chunk, :], preferred_element_type=F32)
    out_ref[...] = acc.astype(BF16)


def call_whole(kernel, operands, out_shape, name, scratch=(), limit=40, smem=()):
    specs = [
        pl.BlockSpec(memory_space=pltpu.SMEM if i in smem else pltpu.VMEM)
        for i in range(len(operands))
    ]
    many = isinstance(out_shape, (list, tuple))
    out_specs = pl.BlockSpec(memory_space=pltpu.VMEM)
    return pl.pallas_call(
        kernel,
        in_specs=specs,
        out_specs=[out_specs] * len(out_shape) if many else out_specs,
        out_shape=out_shape,
        scratch_shapes=list(scratch),
        compiler_params=pltpu.CompilerParams(vmem_limit_bytes=limit * 2**20),
        name=name,
    )(*operands)


def picker():
    row = lax.broadcasted_iota(jnp.int32, (384, 2048), 0)
    col = lax.broadcasted_iota(jnp.int32, (384, 2048), 1)
    tap = col % 128
    hit = (row // 64 == tap // 6) & (row % 64 == 4 * (col // 128) - 1 + tap % 6)
    return hit.astype(BF16)


def per_device(
    density, stem_weight, stem_bias, pos_embed, ln1_gain, ln1_bias, w_qkv, qkv_bias, w_out,
    out_bias, ln2_gain, ln2_bias, w_fc1, fc1_bias, w_fc2, fc2_bias,
):
    axis = "ctx"
    index = lax.axis_index(axis)
    local = jnp.sum(density)
    sums = lax.all_to_all(
        jnp.broadcast_to(local, (32, 1, 1)), axis, split_axis=0, concat_axis=0, tiled=True
    ).reshape(1, 32)
    up = [(i, i + 1) for i in range(31)]
    low = lax.ppermute(density[3:4], axis, up)
    high = lax.ppermute(density[0:1], axis, [(b, a) for a, b in up])
    edge = jnp.stack([index > 0, index < 31]).astype(jnp.int32)
    stem = stem_weight.reshape(36, 6, D).transpose(1, 0, 2)
    stem = jnp.pad(stem, ((0, 0), (0, 12), (0, 0)))
    row = lambda v: v.reshape(1, -1)
    send, residual = call_whole(
        front_kernel,
        (sums, edge, low, density, high, picker(), stem, row(stem_bias), pos_embed,
         row(ln1_gain), row(ln1_bias), w_qkv, row(qkv_bias)),
        [
            jax.ShapeDtypeStruct((PLANE, 3 * HEAD, TOK), BF16),
            jax.ShapeDtypeStruct((TOK, D), BF16),
        ],
        "front",
        scratch=(pltpu.VMEM((SIDE, 80, 128), F32),),
        smem=(1,),
    )
    groups = [list(range(PLANE)), list(range(PLANE, 2 * PLANE))]
    got = lax.all_to_all(
        send, axis, split_axis=0, concat_axis=0, tiled=True, axis_index_groups=groups
    )
    other = lax.ppermute(got[:, : 2 * HEAD, :], axis, [(i, i ^ PLANE) for i in range(32)])
    acc, top = attend((got,), False)
    mixed = attend((got, other, acc, top), True)
    back = lax.all_to_all(
        mixed, axis, split_axis=0, concat_axis=0, tiled=True, axis_index_groups=groups
    )
    return call_whole(
        back_kernel,
        (back.reshape(D, TOK), residual, w_out, row(out_bias), row(ln2_gain), row(ln2_bias),
         w_fc1, row(fc1_bias), w_fc2, row(fc2_bias)),
        jax.ShapeDtypeStruct((TOK, D), BF16),
        "back",
    )


def solution(mesh):
    in_specs = (
        P(("dp", "ctx"), None, None),
        P(), P(),
        P("ctx", None),
        P(), P(), P(), P(), P(), P(), P(), P(), P(), P(), P(), P(),
    )
    return jax.shard_map(
        per_device, mesh=mesh, in_specs=in_specs, out_specs=P(("dp", "ctx"), None), check_vma=False
    )
```

```python
import math

import jax
import jax.numpy as jnp
from jax import lax
from jax.experimental import pallas as pl
from jax.experimental.pallas import tpu as pltpu
from jax.sharding import PartitionSpec as P

HEADS = 16
HEAD = 64
D = 1024
FF = 4096
SIDE = 16
TOK = 256
DEVS = 32
BOUND = 100.0
F32 = jnp.float32
BF16 = jnp.bfloat16


def layer_norm(values, gain, shift):
    center = values - jnp.mean(values, axis=-1, keepdims=True)
    spread = jnp.mean(center * center, axis=-1, keepdims=True)
    return center * lax.rsqrt(spread + 1e-06) * gain + shift


def start_kernel(index_ref, density_ref, out_ref):
    index = index_ref[0]
    total = jnp.sum(density_ref[...]) * jnp.ones((8, 128), F32)

    def packed(plane):
        return jnp.concatenate([plane[:32], plane[32:]], axis=1)

    bottom = packed(density_ref[0])
    for d in range(DEVS):
        out_ref[d, 0:32, :] = bottom
        out_ref[d, 32:40, :] = total

    @pl.when(index < DEVS - 1)
    def _():
        out_ref[index + 1, 0:32, :] = packed(density_ref[3])


def front_kernel(
    index_ref, got_ref, mid_ref, stem_ref, sbias_ref, pos_ref, gain_ref, shift_ref, qbias_ref,
    wqkv_hbm, send_ref, resid_ref, cols_ref, pick_ref, wqkv_ref, sems,
):
    copies = [
        pltpu.make_async_copy(
            wqkv_hbm.at[:, pl.ds(n * 512, 512)], wqkv_ref.at[n], sems.at[n]
        )
        for n in range(6)
    ]
    for copy in copies:
        copy.start()
    index = index_ref[0]
    row = lax.broadcasted_iota(jnp.int32, (64, 2048), 0)
    col = lax.broadcasted_iota(jnp.int32, (64, 2048), 1)
    tap = col % 128
    hit = row == 4 * (col // 128) - 1 + tap % 6
    for a in range(6):
        chosen = jnp.where(tap // 6 == a, jnp.where(hit, 1.0, 0.0), 0.0)
        pick_ref[a * 64 : (a + 1) * 64, :] = chosen.astype(BF16)
    row = lax.broadcasted_iota(jnp.int32, (288, 216), 0)
    col = lax.broadcasted_iota(jnp.int32, (288, 216), 1)
    order = jnp.where((row % 48 < 36) & (col == (row % 48) * 6 + row // 48), 1.0, 0.0)
    stem = jnp.dot(order.astype(BF16), stem_ref[...], preferred_element_type=F32).astype(BF16)

    total = jnp.sum(got_ref[:, 32:33, :], axis=0)
    mean = total[:, 0:64] / (DEVS * 4 * 64 * 64)

    def halo(source, valid):
        block = got_ref[source, 0:32, :]
        plane = jnp.concatenate([block[:, :64], block[:, 64:]], axis=0)
        return jnp.where(valid, plane, mean)

    low = halo(jnp.maximum(index - 1, 0), index > 0)
    high = halo(jnp.minimum(index + 1, DEVS - 1), index < DEVS - 1)
    planes = [low] + [mid_ref[a] for a in range(4)] + [high]
    field = jnp.concatenate([jnp.log(p / mean).astype(BF16) for p in planes], axis=0)
    cols_ref[:, 0:8, :] = jnp.zeros((SIDE, 8, 128), F32)
    cols_ref[:, 72:80, :] = jnp.zeros((SIDE, 8, 128), F32)
    picked = lax.dot_general(
        field, pick_ref[...], (((0,), (0,)), ((), ())), preferred_element_type=F32
    )
    for j in range(SIDE):
        cols_ref[j, 8:72, :] = picked[:, j * 128 : (j + 1) * 128]
    embedded = sbias_ref[...] + pos_ref[...].astype(F32)
    for c in range(6):
        rows = [cols_ref[j, pl.ds(7 + c, SIDE, stride=4), :] for j in range(SIDE)]
        taps = jnp.concatenate(rows, axis=0).astype(BF16)
        embedded = embedded + jnp.dot(
            taps[:, :48], stem[c * 48 : (c + 1) * 48], preferred_element_type=F32
        )
    residual = embedded.astype(BF16)
    resid_ref[...] = residual
    normed = layer_norm(residual.astype(F32), gain_ref[...], shift_ref[...]).astype(BF16)
    scale = math.log2(math.e) / math.sqrt(HEAD)
    for part in range(3):
        for n in range(2):
            start = part * D + n * 512
            copies[part * 2 + n].wait()
            out = jnp.dot(normed, wqkv_ref[part * 2 + n], preferred_element_type=F32)
            out = out + qbias_ref[:, start : start + 512]
            if part == 0:
                out = out * scale
            out = out.astype(BF16)
            for pair in range(4):
                both = out[:, pair * 128 : (pair + 1) * 128].T
                for half in range(2):
                    head = n * 8 + pair * 2 + half
                    block = both[half * HEAD : (half + 1) * HEAD]
                    left, right = block[:, :128], block[:, 128:]
                    if part == 0:
                        send_ref[head, 256:320, :] = left
                        send_ref[head + HEADS, 256:320, :] = right
                    else:
                        base = (part - 1) * 128
                        for g in range(2):
                            send_ref[head + g * HEADS, base : base + 64, :] = left
                            send_ref[head + g * HEADS, base + 64 : base + 128, :] = right


def attend_kernel(got_ref, out_ref, k_scr, v_scr):
    zero = jnp.zeros((1, 128), F32)
    reach_k, reach_q = zero, zero

    def square(block):
        wide = block.astype(F32)
        return jnp.sum(wide * wide, axis=0, keepdims=True)

    for s in range(DEVS):
        key = jnp.concatenate([got_ref[s, 0:64, :], got_ref[s, 64:128, :]], axis=1)
        k_scr[s * TOK : (s + 1) * TOK, :] = key.T
        v_scr[0:HEAD, s * TOK : s * TOK + 128] = got_ref[s, 128:192, :]
        v_scr[0:HEAD, s * TOK + 128 : (s + 1) * TOK] = got_ref[s, 192:256, :]
        reach_k = jnp.maximum(reach_k, square(got_ref[s, 0:64, :]))
        reach_k = jnp.maximum(reach_k, square(got_ref[s, 64:128, :]))
        reach_q = jnp.maximum(reach_q, square(got_ref[s, 256:320, :]))
    v_scr[HEAD : 2 * HEAD, :] = jnp.ones((HEAD, DEVS * TOK), BF16)
    small = jnp.max(reach_k) * jnp.max(reach_q) <= BOUND * BOUND
    width = 512

    def query_of(i):
        return jnp.concatenate([got_ref[4 * i + j, 256:320, :] for j in range(4)], axis=1)

    def finish(i, acc):
        out = (acc[:HEAD] / acc[HEAD : HEAD + 1]).astype(BF16)
        for j in range(4):
            out_ref[4 * i + j] = out[:, j * 128 : (j + 1) * 128]

    @pl.when(small)
    def _():
        def tile(i, _):
            scores = jnp.dot(k_scr[...], query_of(i), preferred_element_type=F32)
            weights = jnp.exp2(scores).astype(BF16)
            finish(i, jnp.dot(v_scr[...], weights, preferred_element_type=F32))
            return 0

        lax.fori_loop(0, 8, tile, 0)

    @pl.when(jnp.logical_not(small))
    def _():
        chunk = 256

        def tile(i, _):
            query = query_of(i)

            def one(c, carry):
                acc, top = carry
                off = pl.multiple_of(c * chunk, chunk)
                scores = jnp.dot(k_scr[pl.ds(off, chunk), :], query, preferred_element_type=F32)
                new_top = jnp.maximum(top, jnp.max(scores, axis=0, keepdims=True))
                weights = jnp.exp2(scores - new_top).astype(BF16)
                acc = acc * jnp.exp2(top - new_top) + jnp.dot(
                    v_scr[0 : HEAD + 16, pl.ds(off, chunk)], weights, preferred_element_type=F32
                )
                return acc, new_top

            begin = (jnp.zeros((HEAD + 16, width), F32), jnp.full((1, width), -3e38, F32))
            acc, _ = lax.fori_loop(0, DEVS * TOK // chunk, one, begin)
            finish(i, acc)
            return 0

        lax.fori_loop(0, 8, tile, 0)


def back_kernel(
    att_ref, resid_ref, wout_ref, obias_ref, gain_ref, shift_ref, fc1_ref, b1_ref, fc2_ref,
    b2_ref, out_ref,
):
    mixed = jnp.concatenate(
        [
            lax.dot_general(
                att_ref[g * HEADS : (g + 1) * HEADS].reshape(D, 128),
                wout_ref[...],
                (((0,), (0,)), ((), ())),
                preferred_element_type=F32,
            )
            for g in range(2)
        ],
        axis=0,
    )
    stream = (resid_ref[...].astype(F32) + mixed + obias_ref[...]).astype(BF16)
    wide = stream.astype(F32)
    normed = layer_norm(wide, gain_ref[...], shift_ref[...]).astype(BF16)
    acc = wide + b2_ref[...]
    chunk = 1024
    for f in range(0, FF, chunk):
        pre = jnp.dot(normed, fc1_ref[:, f : f + chunk], preferred_element_type=F32)
        pre = pre + b1_ref[:, f : f + chunk]
        hidden = (0.5 * pre * (1.0 + lax.erf(pre * math.sqrt(0.5)))).astype(BF16)
        acc = acc + jnp.dot(hidden, fc2_ref[f : f + chunk, :], preferred_element_type=F32)
    out_ref[...] = acc.astype(BF16)


def call_whole(kernel, operands, out_shape, name, limit, scratch=(), smem=(), hbm=()):
    def space(i):
        return pltpu.SMEM if i in smem else pl.ANY if i in hbm else pltpu.VMEM

    specs = [pl.BlockSpec(memory_space=space(i)) for i in range(len(operands))]
    many = isinstance(out_shape, (list, tuple))
    out_specs = pl.BlockSpec(memory_space=pltpu.VMEM)
    return pl.pallas_call(
        kernel,
        in_specs=specs,
        out_specs=[out_specs] * len(out_shape) if many else out_specs,
        out_shape=out_shape,
        scratch_shapes=list(scratch),
        compiler_params=pltpu.CompilerParams(vmem_limit_bytes=limit * 2**20),
        name=name,
    )(*operands)


def per_device(
    density, stem_weight, stem_bias, pos_embed, ln1_gain, ln1_bias, w_qkv, qkv_bias, w_out,
    out_bias, ln2_gain, ln2_bias, w_fc1, fc1_bias, w_fc2, fc2_bias,
):
    row = lambda v: v.reshape(1, -1)
    shape = jax.ShapeDtypeStruct
    everyone = lambda v: lax.all_to_all(v, "ctx", split_axis=0, concat_axis=0, tiled=True)
    index = lax.axis_index("ctx").astype(jnp.int32).reshape(1)
    first = call_whole(
        start_kernel, (index, density), shape((DEVS, 40, 128), F32), "start", 4, smem=(0,)
    )
    got = everyone(first)
    send, residual = call_whole(
        front_kernel,
        (index, got, density, stem_weight, row(stem_bias), pos_embed, row(ln1_gain),
         row(ln1_bias), row(qkv_bias), w_qkv),
        [shape((DEVS, 320, 128), BF16), shape((TOK, D), BF16)],
        "front",
        20,
        scratch=(
            pltpu.VMEM((SIDE, 80, 128), F32),
            pltpu.VMEM((384, 2048), BF16),
            pltpu.VMEM((6, D, 512), BF16),
            pltpu.SemaphoreType.DMA((6,)),
        ),
        smem=(0,),
        hbm=(9,),
    )
    mixed = call_whole(
        attend_kernel,
        (everyone(send),),
        shape((DEVS, HEAD, 128), BF16),
        "attend",
        20,
        scratch=(
            pltpu.VMEM((DEVS * TOK, HEAD), BF16),
            pltpu.VMEM((2 * HEAD, DEVS * TOK), BF16),
        ),
    )
    return call_whole(
        back_kernel,
        (everyone(mixed), residual, w_out, row(out_bias), row(ln2_gain), row(ln2_bias),
         w_fc1, row(fc1_bias), w_fc2, row(fc2_bias)),
        shape((TOK, D), BF16),
        "back",
        16,
    )


def solution(mesh):
    rest = [P()] * 12
    in_specs = (P(("dp", "ctx"), None, None), P(), P(), P("ctx", None), *rest)
    return jax.shard_map(
        per_device, mesh=mesh, in_specs=in_specs, out_specs=P(("dp", "ctx"), None), check_vma=False
    )
```

```python
import math

import jax
import jax.numpy as jnp
from jax import lax
from jax.experimental import pallas as pl
from jax.experimental.pallas import tpu as pltpu
from jax.sharding import PartitionSpec as P

HEADS = 16
HEAD = 64
D = 1024
FF = 4096
SIDE = 16
TOK = 256
DEVS = 32
BOUND = 100.0
F32 = jnp.float32
BF16 = jnp.bfloat16


def layer_norm(values, gain, shift):
    center = values - jnp.mean(values, axis=-1, keepdims=True)
    spread = jnp.mean(center * center, axis=-1, keepdims=True)
    return center * lax.rsqrt(spread + 1e-06) * gain + shift


def start_kernel(index_ref, density_ref, out_ref):
    index = index_ref[0]
    total = jnp.sum(density_ref[...]) * jnp.ones((8, 128), F32)

    def packed(plane):
        return jnp.concatenate([plane[:32], plane[32:]], axis=1)

    bottom = packed(density_ref[0])
    for d in range(DEVS):
        out_ref[d, 0:32, :] = bottom
        out_ref[d, 32:40, :] = total

    @pl.when(index < DEVS - 1)
    def _():
        out_ref[index + 1, 0:32, :] = packed(density_ref[3])


def front_kernel(
    index_ref, got_ref, mid_ref, stem_ref, sbias_ref, pos_ref, gain_ref, shift_ref, qbias_ref,
    wqkv_ref, send_ref, resid_ref, cols_ref, pick_ref,
):
    index = index_ref[0]
    row = lax.broadcasted_iota(jnp.int32, (64, 2048), 0)
    col = lax.broadcasted_iota(jnp.int32, (64, 2048), 1)
    tap = col % 128
    hit = row == 4 * (col // 128) - 1 + tap % 6
    for a in range(6):
        chosen = jnp.where(tap // 6 == a, jnp.where(hit, 1.0, 0.0), 0.0)
        pick_ref[a * 64 : (a + 1) * 64, :] = chosen.astype(BF16)
    row = lax.broadcasted_iota(jnp.int32, (288, 216), 0)
    col = lax.broadcasted_iota(jnp.int32, (288, 216), 1)
    order = jnp.where((row % 48 < 36) & (col == (row % 48) * 6 + row // 48), 1.0, 0.0)
    stem = jnp.dot(order.astype(BF16), stem_ref[...], preferred_element_type=F32).astype(BF16)

    total = jnp.sum(got_ref[:, 32:33, :], axis=0)
    mean = total[:, 0:64] / (DEVS * 4 * 64 * 64)

    def halo(source, valid):
        block = got_ref[source, 0:32, :]
        plane = jnp.concatenate([block[:, :64], block[:, 64:]], axis=0)
        return jnp.where(valid, plane, mean)

    low = halo(jnp.maximum(index - 1, 0), index > 0)
    high = halo(jnp.minimum(index + 1, DEVS - 1), index < DEVS - 1)
    planes = [low] + [mid_ref[a] for a in range(4)] + [high]
    field = jnp.concatenate([jnp.log(p / mean).astype(BF16) for p in planes], axis=0)
    cols_ref[:, 0:8, :] = jnp.zeros((SIDE, 8, 128), F32)
    cols_ref[:, 72:80, :] = jnp.zeros((SIDE, 8, 128), F32)
    picked = lax.dot_general(
        field, pick_ref[...], (((0,), (0,)), ((), ())), preferred_element_type=F32
    )
    for j in range(SIDE):
        cols_ref[j, 8:72, :] = picked[:, j * 128 : (j + 1) * 128]
    embedded = sbias_ref[...] + pos_ref[...].astype(F32)
    for c in range(6):
        rows = [cols_ref[j, pl.ds(7 + c, SIDE, stride=4), :] for j in range(SIDE)]
        taps = jnp.concatenate(rows, axis=0).astype(BF16)
        embedded = embedded + jnp.dot(
            taps[:, :48], stem[c * 48 : (c + 1) * 48], preferred_element_type=F32
        )
    residual = embedded.astype(BF16)
    resid_ref[...] = residual
    normed = layer_norm(residual.astype(F32), gain_ref[...], shift_ref[...]).astype(BF16)
    scale = math.log2(math.e) / math.sqrt(HEAD)
    for part in range(3):
        for n in range(2):
            start = part * D + n * 512
            out = jnp.dot(normed, wqkv_ref[:, start : start + 512], preferred_element_type=F32)
            out = out + qbias_ref[:, start : start + 512]
            if part == 0:
                out = out * scale
            out = out.astype(BF16)
            for pair in range(4):
                both = out[:, pair * 128 : (pair + 1) * 128].T
                for half in range(2):
                    head = n * 8 + pair * 2 + half
                    block = both[half * HEAD : (half + 1) * HEAD]
                    left, right = block[:, :128], block[:, 128:]
                    if part == 0:
                        send_ref[head, 256:320, :] = left
                        send_ref[head + HEADS, 256:320, :] = right
                    else:
                        base = (part - 1) * 128
                        for g in range(2):
                            send_ref[head + g * HEADS, base : base + 64, :] = left
                            send_ref[head + g * HEADS, base + 64 : base + 128, :] = right


def attend_kernel(
    got_ref, wout_hbm, fc1_hbm, fc2_hbm, out_ref, wout_ref, fc1_ref, fc2_ref, k_scr, v_scr, sems,
):
    pairs = ((wout_hbm, wout_ref), (fc1_hbm, fc1_ref), (fc2_hbm, fc2_ref))
    copies = [pltpu.make_async_copy(a, b, sems.at[n]) for n, (a, b) in enumerate(pairs)]
    for copy in copies:
        copy.start()
    zero = jnp.zeros((1, 128), F32)
    reach_k, reach_q = zero, zero

    def square(block):
        wide = block.astype(F32)
        return jnp.sum(wide * wide, axis=0, keepdims=True)

    for s in range(DEVS):
        key = jnp.concatenate([got_ref[s, 0:64, :], got_ref[s, 64:128, :]], axis=1)
        k_scr[s * TOK : (s + 1) * TOK, :] = key.T
        v_scr[0:HEAD, s * TOK : s * TOK + 128] = got_ref[s, 128:192, :]
        v_scr[0:HEAD, s * TOK + 128 : (s + 1) * TOK] = got_ref[s, 192:256, :]
        reach_k = jnp.maximum(reach_k, square(got_ref[s, 0:64, :]))
        reach_k = jnp.maximum(reach_k, square(got_ref[s, 64:128, :]))
        reach_q = jnp.maximum(reach_q, square(got_ref[s, 256:320, :]))
    v_scr[HEAD : 2 * HEAD, :] = jnp.ones((HEAD, DEVS * TOK), BF16)
    small = jnp.max(reach_k) * jnp.max(reach_q) <= BOUND * BOUND
    width = 512

    def query_of(i):
        return jnp.concatenate([got_ref[4 * i + j, 256:320, :] for j in range(4)], axis=1)

    def finish(i, acc):
        out = (acc[:HEAD] / acc[HEAD : HEAD + 1]).astype(BF16)
        for j in range(4):
            out_ref[4 * i + j] = out[:, j * 128 : (j + 1) * 128]

    @pl.when(small)
    def _():
        def tile(i, _):
            scores = jnp.dot(k_scr[...], query_of(i), preferred_element_type=F32)
            weights = jnp.exp2(scores).astype(BF16)
            finish(i, jnp.dot(v_scr[...], weights, preferred_element_type=F32))
            return 0

        lax.fori_loop(0, 8, tile, 0)

    @pl.when(jnp.logical_not(small))
    def _():
        chunk = 256

        def tile(i, _):
            query = query_of(i)

            def one(c, carry):
                acc, top = carry
                off = pl.multiple_of(c * chunk, chunk)
                scores = jnp.dot(k_scr[pl.ds(off, chunk), :], query, preferred_element_type=F32)
                new_top = jnp.maximum(top, jnp.max(scores, axis=0, keepdims=True))
                weights = jnp.exp2(scores - new_top).astype(BF16)
                acc = acc * jnp.exp2(top - new_top) + jnp.dot(
                    v_scr[0 : HEAD + 16, pl.ds(off, chunk)], weights, preferred_element_type=F32
                )
                return acc, new_top

            begin = (jnp.zeros((HEAD + 16, width), F32), jnp.full((1, width), -3e38, F32))
            acc, _ = lax.fori_loop(0, DEVS * TOK // chunk, one, begin)
            finish(i, acc)
            return 0

        lax.fori_loop(0, 8, tile, 0)

    for copy in copies:
        copy.wait()


def back_kernel(
    att_ref, resid_ref, wout_ref, obias_ref, gain_ref, shift_ref, fc1_ref, b1_ref, fc2_ref,
    b2_ref, out_ref,
):
    mixed = jnp.concatenate(
        [
            lax.dot_general(
                att_ref[g * HEADS : (g + 1) * HEADS].reshape(D, 128),
                wout_ref[...],
                (((0,), (0,)), ((), ())),
                preferred_element_type=F32,
            )
            for g in range(2)
        ],
        axis=0,
    )
    stream = (resid_ref[...].astype(F32) + mixed + obias_ref[...]).astype(BF16)
    wide = stream.astype(F32)
    normed = layer_norm(wide, gain_ref[...], shift_ref[...]).astype(BF16)
    acc = wide + b2_ref[...]
    chunk = 1024
    for f in range(0, FF, chunk):
        pre = jnp.dot(normed, fc1_ref[:, f : f + chunk], preferred_element_type=F32)
        pre = pre + b1_ref[:, f : f + chunk]
        hidden = (0.5 * pre * (1.0 + lax.erf(pre * math.sqrt(0.5)))).astype(BF16)
        acc = acc + jnp.dot(hidden, fc2_ref[f : f + chunk, :], preferred_element_type=F32)
    out_ref[...] = acc.astype(BF16)


def call_whole(kernel, operands, out_shape, name, limit, scratch=(), smem=(), hbm=(), giga=1):
    def space(i):
        return pltpu.SMEM if i in smem else pltpu.HBM if i in hbm else pltpu.VMEM

    specs = [pl.BlockSpec(memory_space=space(i)) for i in range(len(operands))]
    many = isinstance(out_shape, (list, tuple))
    out_specs = pl.BlockSpec(memory_space=pltpu.VMEM)
    return pl.pallas_call(
        kernel,
        in_specs=specs,
        out_specs=[out_specs] * len(out_shape) if many else out_specs,
        out_shape=out_shape,
        scratch_shapes=list(scratch),
        compiler_params=pltpu.CompilerParams(vmem_limit_bytes=limit * 2**20),
        cost_estimate=pl.CostEstimate(
            flops=giga * 10**9, bytes_accessed=10**6, transcendentals=0
        ),
        name=name,
    )(*operands)


def per_device(
    density, stem_weight, stem_bias, pos_embed, ln1_gain, ln1_bias, w_qkv, qkv_bias, w_out,
    out_bias, ln2_gain, ln2_bias, w_fc1, fc1_bias, w_fc2, fc2_bias,
):
    row = lambda v: v.reshape(1, -1)
    shape = jax.ShapeDtypeStruct
    everyone = lambda v: lax.all_to_all(v, "ctx", split_axis=0, concat_axis=0, tiled=True)
    index = lax.axis_index("ctx").astype(jnp.int32).reshape(1)
    first = call_whole(
        start_kernel, (index, density), shape((DEVS, 40, 128), F32), "start", 4, smem=(0,),
        giga=20,
    )
    got = everyone(first)
    send, residual = call_whole(
        front_kernel,
        (index, got, density, stem_weight, row(stem_bias), pos_embed, row(ln1_gain),
         row(ln1_bias), row(qkv_bias), w_qkv),
        [shape((DEVS, 320, 128), BF16), shape((TOK, D), BF16)],
        "front",
        20,
        scratch=(
            pltpu.VMEM((SIDE, 80, 128), F32),
            pltpu.VMEM((384, 2048), BF16),
        ),
        smem=(0,),
    )
    mixed, w_out, w_fc1, w_fc2 = call_whole(
        attend_kernel,
        (everyone(send), w_out, w_fc1, w_fc2),
        [
            shape((DEVS, HEAD, 128), BF16),
            shape(w_out.shape, BF16),
            shape(w_fc1.shape, BF16),
            shape(w_fc2.shape, BF16),
        ],
        "attend",
        24,
        scratch=(
            pltpu.VMEM((DEVS * TOK, HEAD), BF16),
            pltpu.VMEM((2 * HEAD, DEVS * TOK), BF16),
            pltpu.SemaphoreType.DMA((3,)),
        ),
        hbm=(1, 2, 3),
        giga=28,
    )
    return call_whole(
        back_kernel,
        (everyone(mixed), residual, w_out, row(out_bias), row(ln2_gain), row(ln2_bias),
         w_fc1, row(fc1_bias), w_fc2, row(fc2_bias)),
        shape((TOK, D), BF16),
        "back",
        16,
    )


def solution(mesh):
    rest = [P()] * 12
    in_specs = (P(("dp", "ctx"), None, None), P(), P(), P("ctx", None), *rest)
    return jax.shard_map(
        per_device, mesh=mesh, in_specs=in_specs, out_specs=P(("dp", "ctx"), None), check_vma=False
    )
```

```python
import math

import jax
import jax.numpy as jnp
from jax import lax
from jax.experimental import pallas as pl
from jax.experimental.pallas import tpu as pltpu
from jax.sharding import PartitionSpec as P

HEADS = 16
HEAD = 64
D = 1024
FF = 4096
SIDE = 16
TOK = 256
DEVS = 32
VOXELS = 4 * 64 * 64
BOUND = 100.0
F32 = jnp.float32
BF16 = jnp.bfloat16


def layer_norm(values, gain, shift):
    center = values - jnp.mean(values, axis=-1, keepdims=True)
    spread = jnp.mean(center * center, axis=-1, keepdims=True)
    return center * lax.rsqrt(spread + 1e-06) * gain + shift


def start_kernel(index_ref, density_ref, out_ref):
    index = index_ref[0]
    total = jnp.sum(density_ref[...]) * jnp.ones((16, 128), F32)
    local = total[0:1, :64] / VOXELS
    high = total.astype(BF16)
    left = total - high.astype(F32)
    middle = left.astype(BF16)
    low = (left - middle.astype(F32)).astype(BF16)
    row = lax.broadcasted_iota(jnp.int32, (16, 128), 0)
    pieces = jnp.where(row == 0, high.astype(F32), 0.0)
    pieces = jnp.where(row == 1, middle.astype(F32), pieces)
    pieces = jnp.where(row == 2, low.astype(F32), pieces).astype(BF16)

    def packed(plane):
        field = jnp.log(plane / local)
        return jnp.concatenate([field[:32], field[32:]], axis=1).astype(BF16)

    bottom = packed(density_ref[0])
    for d in range(DEVS):
        out_ref[d, 0:32, :] = bottom
        out_ref[d, 32:48, :] = pieces

    @pl.when(index < DEVS - 1)
    def _():
        out_ref[index + 1, 0:32, :] = packed(density_ref[3])


def front_kernel(
    index_ref, got_ref, mid_ref, stem_ref, sbias_ref, pos_ref, gain_ref, shift_ref, qbias_ref,
    wqkv_ref, send_ref, resid_ref, cols_ref, pick_ref,
):
    index = index_ref[0]
    row = lax.broadcasted_iota(jnp.int32, (64, 2048), 0)
    col = lax.broadcasted_iota(jnp.int32, (64, 2048), 1)
    tap = col % 128
    hit = row == 4 * (col // 128) - 1 + tap % 6
    for a in range(6):
        chosen = jnp.where(tap // 6 == a, jnp.where(hit, 1.0, 0.0), 0.0)
        pick_ref[a * 64 : (a + 1) * 64, :] = chosen.astype(BF16)
    row = lax.broadcasted_iota(jnp.int32, (288, 216), 0)
    col = lax.broadcasted_iota(jnp.int32, (288, 216), 1)
    order = jnp.where((row % 48 < 36) & (col == (row % 48) * 6 + row // 48), 1.0, 0.0)
    stem = jnp.dot(order.astype(BF16), stem_ref[...], preferred_element_type=F32).astype(BF16)

    sums = jnp.sum(got_ref[:, 32:48, :].astype(F32), axis=1)
    mean = jnp.sum(sums, axis=0, keepdims=True)[:, :64] / (DEVS * VOXELS)

    def halo(source, valid):
        block = got_ref[source, 0:32, :].astype(F32)
        plane = jnp.concatenate([block[:, :64], block[:, 64:]], axis=0)
        local = jnp.sum(got_ref[source, 32:48, :].astype(F32), axis=0, keepdims=True)
        shift = jnp.log(local[:, :64] / VOXELS / mean)
        return jnp.where(valid, plane + shift, 0.0).astype(BF16)

    low = halo(jnp.maximum(index - 1, 0), index > 0)
    high = halo(jnp.minimum(index + 1, DEVS - 1), index < DEVS - 1)
    planes = [low] + [jnp.log(mid_ref[a] / mean).astype(BF16) for a in range(4)] + [high]
    field = jnp.concatenate(planes, axis=0)
    cols_ref[:, 0:8, :] = jnp.zeros((SIDE, 8, 128), F32)
    cols_ref[:, 72:80, :] = jnp.zeros((SIDE, 8, 128), F32)
    picked = lax.dot_general(
        field, pick_ref[...], (((0,), (0,)), ((), ())), preferred_element_type=F32
    )
    for j in range(SIDE):
        cols_ref[j, 8:72, :] = picked[:, j * 128 : (j + 1) * 128]
    embedded = sbias_ref[...] + pos_ref[...].astype(F32)
    for c in range(6):
        rows = [cols_ref[j, pl.ds(7 + c, SIDE, stride=4), :] for j in range(SIDE)]
        taps = jnp.concatenate(rows, axis=0).astype(BF16)
        embedded = embedded + jnp.dot(
            taps[:, :48], stem[c * 48 : (c + 1) * 48], preferred_element_type=F32
        )
    residual = embedded.astype(BF16)
    resid_ref[...] = residual
    normed = layer_norm(residual.astype(F32), gain_ref[...], shift_ref[...]).astype(BF16)
    scale = math.log2(math.e) / math.sqrt(HEAD)
    for part in range(3):
        for n in range(2):
            start = part * D + n * 512
            out = jnp.dot(normed, wqkv_ref[:, start : start + 512], preferred_element_type=F32)
            out = out + qbias_ref[:, start : start + 512]
            if part == 0:
                out = out * scale
            out = out.astype(BF16)
            for pair in range(4):
                both = out[:, pair * 128 : (pair + 1) * 128].T
                for half in range(2):
                    head = n * 8 + pair * 2 + half
                    block = both[half * HEAD : (half + 1) * HEAD]
                    left, right = block[:, :128], block[:, 128:]
                    if part == 0:
                        send_ref[head, 256:320, :] = left
                        send_ref[head + HEADS, 256:320, :] = right
                    else:
                        base = (part - 1) * 128
                        for g in range(2):
                            send_ref[head + g * HEADS, base : base + 64, :] = left
                            send_ref[head + g * HEADS, base + 64 : base + 128, :] = right


def attend_kernel(
    got_ref, wout_hbm, fc1_hbm, fc2_hbm, out_ref, wout_ref, fc1_ref, fc2_ref, k_scr, v_scr, sems,
):
    pairs = ((wout_hbm, wout_ref), (fc1_hbm, fc1_ref), (fc2_hbm, fc2_ref))
    copies = [pltpu.make_async_copy(a, b, sems.at[n]) for n, (a, b) in enumerate(pairs)]
    for copy in copies:
        copy.start()
    zero = jnp.zeros((1, 128), F32)
    reach_k, reach_q = zero, zero

    def square(block):
        wide = block.astype(F32)
        return jnp.sum(wide * wide, axis=0, keepdims=True)

    for s in range(DEVS):
        key = jnp.concatenate([got_ref[s, 0:64, :], got_ref[s, 64:128, :]], axis=1)
        k_scr[s * TOK : (s + 1) * TOK, :] = key.T
        v_scr[0:HEAD, s * TOK : s * TOK + 128] = got_ref[s, 128:192, :]
        v_scr[0:HEAD, s * TOK + 128 : (s + 1) * TOK] = got_ref[s, 192:256, :]
        reach_k = jnp.maximum(reach_k, square(got_ref[s, 0:64, :]))
        reach_k = jnp.maximum(reach_k, square(got_ref[s, 64:128, :]))
        reach_q = jnp.maximum(reach_q, square(got_ref[s, 256:320, :]))
    v_scr[HEAD : 2 * HEAD, :] = jnp.ones((HEAD, DEVS * TOK), BF16)
    small = jnp.max(reach_k) * jnp.max(reach_q) <= BOUND * BOUND
    width = 512

    def query_of(i):
        return jnp.concatenate([got_ref[4 * i + j, 256:320, :] for j in range(4)], axis=1)

    def finish(i, acc):
        out = (acc[:HEAD] / acc[HEAD : HEAD + 1]).astype(BF16)
        for j in range(4):
            out_ref[4 * i + j] = out[:, j * 128 : (j + 1) * 128]

    @pl.when(small)
    def _():
        def tile(i, _):
            scores = jnp.dot(k_scr[...], query_of(i), preferred_element_type=F32)
            weights = jnp.exp2(scores).astype(BF16)
            finish(i, jnp.dot(v_scr[...], weights, preferred_element_type=F32))
            return 0

        lax.fori_loop(0, 8, tile, 0)

    @pl.when(jnp.logical_not(small))
    def _():
        chunk = 256

        def tile(i, _):
            query = query_of(i)

            def one(c, carry):
                acc, top = carry
                off = pl.multiple_of(c * chunk, chunk)
                scores = jnp.dot(k_scr[pl.ds(off, chunk), :], query, preferred_element_type=F32)
                new_top = jnp.maximum(top, jnp.max(scores, axis=0, keepdims=True))
                weights = jnp.exp2(scores - new_top).astype(BF16)
                acc = acc * jnp.exp2(top - new_top) + jnp.dot(
                    v_scr[0 : HEAD + 16, pl.ds(off, chunk)], weights, preferred_element_type=F32
                )
                return acc, new_top

            begin = (jnp.zeros((HEAD + 16, width), F32), jnp.full((1, width), -3e38, F32))
            acc, _ = lax.fori_loop(0, DEVS * TOK // chunk, one, begin)
            finish(i, acc)
            return 0

        lax.fori_loop(0, 8, tile, 0)

    for copy in copies:
        copy.wait()


def back_kernel(
    att_ref, resid_ref, wout_ref, obias_ref, gain_ref, shift_ref, fc1_ref, b1_ref, fc2_ref,
    b2_ref, out_ref,
):
    mixed = jnp.concatenate(
        [
            lax.dot_general(
                att_ref[g * HEADS : (g + 1) * HEADS].reshape(D, 128),
                wout_ref[...],
                (((0,), (0,)), ((), ())),
                preferred_element_type=F32,
            )
            for g in range(2)
        ],
        axis=0,
    )
    stream = (resid_ref[...].astype(F32) + mixed + obias_ref[...]).astype(BF16)
    wide = stream.astype(F32)
    normed = layer_norm(wide, gain_ref[...], shift_ref[...]).astype(BF16)
    acc = wide + b2_ref[...]
    chunk = 1024
    for f in range(0, FF, chunk):
        pre = jnp.dot(normed, fc1_ref[:, f : f + chunk], preferred_element_type=F32)
        pre = pre + b1_ref[:, f : f + chunk]
        hidden = (0.5 * pre * (1.0 + lax.erf(pre * math.sqrt(0.5)))).astype(BF16)
        acc = acc + jnp.dot(hidden, fc2_ref[f : f + chunk, :], preferred_element_type=F32)
    out_ref[...] = acc.astype(BF16)


def call_whole(kernel, operands, out_shape, name, limit, scratch=(), smem=(), hbm=(), giga=1):
    def space(i):
        return pltpu.SMEM if i in smem else pltpu.HBM if i in hbm else pltpu.VMEM

    specs = [pl.BlockSpec(memory_space=space(i)) for i in range(len(operands))]
    many = isinstance(out_shape, (list, tuple))
    out_specs = pl.BlockSpec(memory_space=pltpu.VMEM)
    return pl.pallas_call(
        kernel,
        in_specs=specs,
        out_specs=[out_specs] * len(out_shape) if many else out_specs,
        out_shape=out_shape,
        scratch_shapes=list(scratch),
        compiler_params=pltpu.CompilerParams(vmem_limit_bytes=limit * 2**20),
        cost_estimate=pl.CostEstimate(
            flops=giga * 10**9, bytes_accessed=10**6, transcendentals=0
        ),
        name=name,
    )(*operands)


def per_device(
    density, stem_weight, stem_bias, pos_embed, ln1_gain, ln1_bias, w_qkv, qkv_bias, w_out,
    out_bias, ln2_gain, ln2_bias, w_fc1, fc1_bias, w_fc2, fc2_bias,
):
    row = lambda v: v.reshape(1, -1)
    shape = jax.ShapeDtypeStruct
    everyone = lambda v: lax.all_to_all(v, "ctx", split_axis=0, concat_axis=0, tiled=True)
    index = lax.axis_index("ctx").astype(jnp.int32).reshape(1)
    first = call_whole(
        start_kernel, (index, density), shape((DEVS, 48, 128), BF16), "start", 4, smem=(0,),
        giga=20,
    )
    got = everyone(first)
    send, residual = call_whole(
        front_kernel,
        (index, got, density, stem_weight, row(stem_bias), pos_embed, row(ln1_gain),
         row(ln1_bias), row(qkv_bias), w_qkv),
        [shape((DEVS, 320, 128), BF16), shape((TOK, D), BF16)],
        "front",
        20,
        scratch=(
            pltpu.VMEM((SIDE, 80, 128), F32),
            pltpu.VMEM((384, 2048), BF16),
        ),
        smem=(0,),
    )
    mixed, w_out, w_fc1, w_fc2 = call_whole(
        attend_kernel,
        (everyone(send), w_out, w_fc1, w_fc2),
        [
            shape((DEVS, HEAD, 128), BF16),
            shape(w_out.shape, BF16),
            shape(w_fc1.shape, BF16),
            shape(w_fc2.shape, BF16),
        ],
        "attend",
        24,
        scratch=(
            pltpu.VMEM((DEVS * TOK, HEAD), BF16),
            pltpu.VMEM((2 * HEAD, DEVS * TOK), BF16),
            pltpu.SemaphoreType.DMA((3,)),
        ),
        hbm=(1, 2, 3),
        giga=28,
    )
    return call_whole(
        back_kernel,
        (everyone(mixed), residual, w_out, row(out_bias), row(ln2_gain), row(ln2_bias),
         w_fc1, row(fc1_bias), w_fc2, row(fc2_bias)),
        shape((TOK, D), BF16),
        "back",
        16,
    )


def solution(mesh):
    rest = [P()] * 12
    in_specs = (P(("dp", "ctx"), None, None), P(), P(), P("ctx", None), *rest)
    return jax.shard_map(
        per_device, mesh=mesh, in_specs=in_specs, out_specs=P(("dp", "ctx"), None), check_vma=False
    )
```

```python
import math

import jax
import jax.numpy as jnp
from jax import lax
from jax.experimental import pallas as pl
from jax.experimental.pallas import tpu as pltpu
from jax.sharding import PartitionSpec as P

HEADS = 16
HEAD = 64
D = 1024
FF = 4096
SIDE = 16
TOK = 256
DEVS = 32
VOXELS = 4 * 64 * 64
BOUND = 100.0
F32 = jnp.float32
BF16 = jnp.bfloat16


def layer_norm(values, gain, shift):
    center = values - jnp.mean(values, axis=-1, keepdims=True)
    spread = jnp.mean(center * center, axis=-1, keepdims=True)
    return center * lax.rsqrt(spread + 1e-06) * gain + shift


def start_kernel(index_ref, density_ref, out_ref):
    index = index_ref[0]
    total = jnp.sum(density_ref[...]) * jnp.ones((8, 128), F32)
    local = total[0:1, :64] / VOXELS
    high = total.astype(BF16)
    left = total - high.astype(F32)
    middle = left.astype(BF16)
    low = (left - middle.astype(F32)).astype(BF16)
    row = lax.broadcasted_iota(jnp.int32, (8, 128), 0)
    pieces = jnp.where(row == 0, high.astype(F32), 0.0)
    pieces = jnp.where(row == 1, middle.astype(F32), pieces)
    pieces = jnp.where(row == 2, low.astype(F32), pieces).astype(BF16)

    def packed(plane):
        field = jnp.log(plane / local)
        return jnp.concatenate([field[:32], field[32:]], axis=1).astype(BF16)

    bottom = packed(density_ref[0])
    for d in range(DEVS):
        out_ref[d, 0:32, :] = bottom
        out_ref[d, 32:40, :] = pieces

    @pl.when(index < DEVS - 1)
    def _():
        out_ref[index + 1, 0:32, :] = packed(density_ref[3])


def front_kernel(
    index_ref, got_ref, mid_ref, stem_ref, sbias_ref, pos_ref, gain_ref, shift_ref, qbias_ref,
    wqkv_ref, send_ref, resid_ref, cols_ref, pick_ref,
):
    index = index_ref[0]
    row = lax.broadcasted_iota(jnp.int32, (64, 2048), 0)
    col = lax.broadcasted_iota(jnp.int32, (64, 2048), 1)
    tap = col % 128
    hit = row == 4 * (col // 128) - 1 + tap % 6
    for a in range(6):
        chosen = jnp.where(tap // 6 == a, jnp.where(hit, 1.0, 0.0), 0.0)
        pick_ref[a * 64 : (a + 1) * 64, :] = chosen.astype(BF16)
    row = lax.broadcasted_iota(jnp.int32, (288, 216), 0)
    col = lax.broadcasted_iota(jnp.int32, (288, 216), 1)
    order = jnp.where((row % 48 < 36) & (col == (row % 48) * 6 + row // 48), 1.0, 0.0)
    stem = jnp.dot(order.astype(BF16), stem_ref[...], preferred_element_type=F32).astype(BF16)

    sums = jnp.sum(got_ref[:, 32:40, :].astype(F32), axis=1)
    mean = jnp.sum(sums, axis=0, keepdims=True)[:, :64] / (DEVS * VOXELS)

    def halo(source, valid):
        block = got_ref[source, 0:32, :].astype(F32)
        plane = jnp.concatenate([block[:, :64], block[:, 64:]], axis=0)
        local = jnp.sum(got_ref[source, 32:40, :].astype(F32), axis=0, keepdims=True)
        shift = jnp.log(local[:, :64] / VOXELS / mean)
        return jnp.where(valid, plane + shift, 0.0).astype(BF16)

    low = halo(jnp.maximum(index - 1, 0), index > 0)
    high = halo(jnp.minimum(index + 1, DEVS - 1), index < DEVS - 1)
    planes = [low] + [jnp.log(mid_ref[a] / mean).astype(BF16) for a in range(4)] + [high]
    field = jnp.concatenate(planes, axis=0)
    cols_ref[:, 0:8, :] = jnp.zeros((SIDE, 8, 128), F32)
    cols_ref[:, 72:80, :] = jnp.zeros((SIDE, 8, 128), F32)
    picked = lax.dot_general(
        field, pick_ref[...], (((0,), (0,)), ((), ())), preferred_element_type=F32
    )
    for j in range(SIDE):
        cols_ref[j, 8:72, :] = picked[:, j * 128 : (j + 1) * 128]
    embedded = sbias_ref[...] + pos_ref[...].astype(F32)
    for c in range(6):
        rows = [cols_ref[j, pl.ds(7 + c, SIDE, stride=4), :] for j in range(SIDE)]
        taps = jnp.concatenate(rows, axis=0).astype(BF16)
        embedded = embedded + jnp.dot(
            taps[:, :48], stem[c * 48 : (c + 1) * 48], preferred_element_type=F32
        )
    residual = embedded.astype(BF16)
    resid_ref[...] = residual
    normed = layer_norm(residual.astype(F32), gain_ref[...], shift_ref[...]).astype(BF16)
    scale = math.log2(math.e) / math.sqrt(HEAD)
    for part in range(3):
        for n in range(2):
            start = part * D + n * 512
            out = jnp.dot(normed, wqkv_ref[:, start : start + 512], preferred_element_type=F32)
            out = out + qbias_ref[:, start : start + 512]
            if part == 0:
                out = out * scale
            out = out.astype(BF16)
            for pair in range(4):
                both = out[:, pair * 128 : (pair + 1) * 128].T
                for half in range(2):
                    head = n * 8 + pair * 2 + half
                    block = both[half * HEAD : (half + 1) * HEAD]
                    left, right = block[:, :128], block[:, 128:]
                    if part == 0:
                        send_ref[head, 256:320, :] = left
                        send_ref[head + HEADS, 256:320, :] = right
                    else:
                        base = (part - 1) * 128
                        for g in range(2):
                            send_ref[head + g * HEADS, base : base + 64, :] = left
                            send_ref[head + g * HEADS, base + 64 : base + 128, :] = right


def attend_kernel(
    got_ref, wout_hbm, fc1_hbm, fc2_hbm, out_ref, wout_ref, fc1_ref, fc2_ref, k_scr, v_scr, sems,
):
    pairs = ((wout_hbm, wout_ref), (fc1_hbm, fc1_ref), (fc2_hbm, fc2_ref))
    copies = [pltpu.make_async_copy(a, b, sems.at[n]) for n, (a, b) in enumerate(pairs)]
    for copy in copies:
        copy.start()
    zero = jnp.zeros((1, 128), F32)
    reach_k, reach_q = zero, zero

    def square(block):
        wide = block.astype(F32)
        return jnp.sum(wide * wide, axis=0, keepdims=True)

    for s in range(DEVS):
        key = jnp.concatenate([got_ref[s, 0:64, :], got_ref[s, 64:128, :]], axis=1)
        k_scr[s * TOK : (s + 1) * TOK, :] = key.T
        v_scr[0:HEAD, s * TOK : s * TOK + 128] = got_ref[s, 128:192, :]
        v_scr[0:HEAD, s * TOK + 128 : (s + 1) * TOK] = got_ref[s, 192:256, :]
        reach_k = jnp.maximum(reach_k, square(got_ref[s, 0:64, :]))
        reach_k = jnp.maximum(reach_k, square(got_ref[s, 64:128, :]))
        reach_q = jnp.maximum(reach_q, square(got_ref[s, 256:320, :]))
    v_scr[HEAD : 2 * HEAD, :] = jnp.ones((HEAD, DEVS * TOK), BF16)
    small = jnp.max(reach_k) * jnp.max(reach_q) <= BOUND * BOUND
    width = 512

    def query_of(i):
        return jnp.concatenate([got_ref[4 * i + j, 256:320, :] for j in range(4)], axis=1)

    def finish(i, acc):
        out = (acc[:HEAD] / acc[HEAD : HEAD + 1]).astype(BF16)
        for j in range(4):
            out_ref[4 * i + j] = out[:, j * 128 : (j + 1) * 128]

    @pl.when(small)
    def _():
        def tile(i, _):
            scores = jnp.dot(k_scr[...], query_of(i), preferred_element_type=F32)
            weights = jnp.exp2(scores).astype(BF16)
            finish(i, jnp.dot(v_scr[...], weights, preferred_element_type=F32))
            return 0

        lax.fori_loop(0, 8, tile, 0)

    @pl.when(jnp.logical_not(small))
    def _():
        chunk = 256

        def tile(i, _):
            query = query_of(i)

            def one(c, carry):
                acc, top = carry
                off = pl.multiple_of(c * chunk, chunk)
                scores = jnp.dot(k_scr[pl.ds(off, chunk), :], query, preferred_element_type=F32)
                new_top = jnp.maximum(top, jnp.max(scores, axis=0, keepdims=True))
                weights = jnp.exp2(scores - new_top).astype(BF16)
                acc = acc * jnp.exp2(top - new_top) + jnp.dot(
                    v_scr[0 : HEAD + 16, pl.ds(off, chunk)], weights, preferred_element_type=F32
                )
                return acc, new_top

            begin = (jnp.zeros((HEAD + 16, width), F32), jnp.full((1, width), -3e38, F32))
            acc, _ = lax.fori_loop(0, DEVS * TOK // chunk, one, begin)
            finish(i, acc)
            return 0

        lax.fori_loop(0, 8, tile, 0)

    for copy in copies:
        copy.wait()


def back_kernel(
    att_ref, resid_ref, wout_ref, obias_ref, gain_ref, shift_ref, fc1_ref, b1_ref, fc2_ref,
    b2_ref, out_ref,
):
    mixed = jnp.concatenate(
        [
            lax.dot_general(
                att_ref[g * HEADS : (g + 1) * HEADS].reshape(D, 128),
                wout_ref[...],
                (((0,), (0,)), ((), ())),
                preferred_element_type=F32,
            )
            for g in range(2)
        ],
        axis=0,
    )
    stream = (resid_ref[...].astype(F32) + mixed + obias_ref[...]).astype(BF16)
    wide = stream.astype(F32)
    normed = layer_norm(wide, gain_ref[...], shift_ref[...]).astype(BF16)
    acc = wide + b2_ref[...]
    chunk = 1024
    for f in range(0, FF, chunk):
        pre = jnp.dot(normed, fc1_ref[:, f : f + chunk], preferred_element_type=F32)
        pre = pre + b1_ref[:, f : f + chunk]
        hidden = (0.5 * pre * (1.0 + lax.erf(pre * math.sqrt(0.5)))).astype(BF16)
        acc = acc + jnp.dot(hidden, fc2_ref[f : f + chunk, :], preferred_element_type=F32)
    out_ref[...] = acc.astype(BF16)


def call_whole(kernel, operands, out_shape, name, limit, scratch=(), smem=(), hbm=(), giga=1):
    def space(i):
        return pltpu.SMEM if i in smem else pltpu.HBM if i in hbm else pltpu.VMEM

    specs = [pl.BlockSpec(memory_space=space(i)) for i in range(len(operands))]
    many = isinstance(out_shape, (list, tuple))
    out_specs = pl.BlockSpec(memory_space=pltpu.VMEM)
    return pl.pallas_call(
        kernel,
        in_specs=specs,
        out_specs=[out_specs] * len(out_shape) if many else out_specs,
        out_shape=out_shape,
        scratch_shapes=list(scratch),
        compiler_params=pltpu.CompilerParams(vmem_limit_bytes=limit * 2**20),
        cost_estimate=pl.CostEstimate(
            flops=giga * 10**9, bytes_accessed=10**6, transcendentals=0
        ),
        name=name,
    )(*operands)


def per_device(
    density, stem_weight, stem_bias, pos_embed, ln1_gain, ln1_bias, w_qkv, qkv_bias, w_out,
    out_bias, ln2_gain, ln2_bias, w_fc1, fc1_bias, w_fc2, fc2_bias,
):
    row = lambda v: v.reshape(1, -1)
    shape = jax.ShapeDtypeStruct
    everyone = lambda v: lax.all_to_all(v, "ctx", split_axis=0, concat_axis=0, tiled=True)
    index = lax.axis_index("ctx").astype(jnp.int32).reshape(1)
    first = call_whole(
        start_kernel, (index, density), shape((DEVS, 40, 128), BF16), "start", 4, smem=(0,),
        giga=20,
    )
    got = everyone(first)
    send, residual = call_whole(
        front_kernel,
        (index, got, density, stem_weight, row(stem_bias), pos_embed, row(ln1_gain),
         row(ln1_bias), row(qkv_bias), w_qkv),
        [shape((DEVS, 320, 128), BF16), shape((TOK, D), BF16)],
        "front",
        20,
        scratch=(
            pltpu.VMEM((SIDE, 80, 128), F32),
            pltpu.VMEM((384, 2048), BF16),
        ),
        smem=(0,),
    )
    mixed, w_out, w_fc1, w_fc2 = call_whole(
        attend_kernel,
        (everyone(send), w_out, w_fc1, w_fc2),
        [
            shape((DEVS, HEAD, 128), BF16),
            shape(w_out.shape, BF16),
            shape(w_fc1.shape, BF16),
            shape(w_fc2.shape, BF16),
        ],
        "attend",
        24,
        scratch=(
            pltpu.VMEM((DEVS * TOK, HEAD), BF16),
            pltpu.VMEM((2 * HEAD, DEVS * TOK), BF16),
            pltpu.SemaphoreType.DMA((3,)),
        ),
        hbm=(1, 2, 3),
        giga=28,
    )
    return call_whole(
        back_kernel,
        (everyone(mixed), residual, w_out, row(out_bias), row(ln2_gain), row(ln2_bias),
         w_fc1, row(fc1_bias), w_fc2, row(fc2_bias)),
        shape((TOK, D), BF16),
        "back",
        16,
    )


def solution(mesh):
    rest = [P()] * 12
    in_specs = (P(("dp", "ctx"), None, None), P(), P(), P("ctx", None), *rest)
    return jax.shard_map(
        per_device, mesh=mesh, in_specs=in_specs, out_specs=P(("dp", "ctx"), None), check_vma=False
    )
```
